16 devices in a mesh: tp: 4 (over z, y), cp: 4 (over x, core).
Axes of the slice: x: 2, y: 2, z: 2, core: 2. Of those that a mesh axis runs over, the one named last changes fastest.
Arguments:
- x_in: bfloat16 [8192, 2048], P('cp')
- positions: int32 [8192], P('cp')
- attn_gain: bfloat16 [2, 2048], replicated
- mlp_gain: bfloat16 [2, 2048], replicated
- w_query: bfloat16 [2, 2048, 2048], P(None, None, 'tp')
- b_query: bfloat16 [2, 2048], P(None, 'tp')
- w_key: bfloat16 [2, 2048, 2048], P(None, None, 'tp')
- b_key: bfloat16 [2, 2048], P(None, 'tp')
- w_value: bfloat16 [2, 2048, 2048], P(None, None, 'tp')
- b_value: bfloat16 [2, 2048], P(None, 'tp')
- w_out: bfloat16 [2, 2048, 2048], P(None, 'tp')
- w_gate: bfloat16 [2, 2048, 5504], P(None, None, 'tp')
- w_up: bfloat16 [2, 2048, 5504], P(None, None, 'tp')
- w_down: bfloat16 [2, 5504, 2048], P(None, 'tp')
Outputs:
- output 1: bfloat16 [8192, 2048], P('cp')
- output 2: bfloat16 [8192, 16, 128], P('cp', 'tp')
- output 3: bfloat16 [8192, 16, 128], P('cp', 'tp')
- output 4: bfloat16 [8192, 16, 128], P('cp', 'tp')
- output 5: bfloat16 [8192, 16, 128], P('cp', 'tp')
All inputs are finite; a program needn't handle non-finite values.
Results may differ from the reference program's by a relative error of at most 0.02.
Values are sent between devices in bfloat16 or wider.
A program may use at most 1 GiB of HBM per device.

```python
import jax
import jax.numpy as jnp
from jax import lax

TOKENS = 8192
HIDDEN = 2048
Q_HEADS = 16
KV_HEADS = 16
HEAD_DIM = 128
FFN_DIM = 5504
WINDOW = 4096


def setup_inputs(seed: int = 0) -> dict:
    key_list = jax.random.split(jax.random.key(seed), 14)
    q_width = Q_HEADS * HEAD_DIM
    kv_width = KV_HEADS * HEAD_DIM

    def normal_draw(key_idx, arr_shape, factor):
        return (jax.random.normal(key_list[key_idx], arr_shape, jnp.float32) * factor).astype(jnp.bfloat16)

    def gain_draw(key_idx):
        return jax.random.uniform(key_list[key_idx], (2, HIDDEN), jnp.float32, 0.5, 1.5).astype(jnp.bfloat16)

    pos_start = jax.random.randint(key_list[1], (), 0, 8192, jnp.int32)
    return {
        'x_in': normal_draw(0, (TOKENS, HIDDEN), 1.0),
        'positions': pos_start + jnp.arange(TOKENS, dtype=jnp.int32),
        'attn_gain': gain_draw(2),
        'mlp_gain': gain_draw(3),
        'w_query': normal_draw(4, (2, HIDDEN, q_width), 2.0 * HIDDEN ** -0.5),
        'b_query': normal_draw(5, (2, q_width), 0.5),
        'w_key': normal_draw(6, (2, HIDDEN, kv_width), 2.0 * HIDDEN ** -0.5),
        'b_key': normal_draw(7, (2, kv_width), 0.5),
        'w_value': normal_draw(8, (2, HIDDEN, kv_width), HIDDEN ** -0.5),
        'b_value': normal_draw(9, (2, kv_width), 0.5),
        'w_out': normal_draw(10, (2, q_width, HIDDEN), 2.0 * q_width ** -0.5),
        'w_gate': normal_draw(11, (2, HIDDEN, FFN_DIM), HIDDEN ** -0.5),
        'w_up': normal_draw(12, (2, HIDDEN, FFN_DIM), HIDDEN ** -0.5),
        'w_down': normal_draw(13, (2, FFN_DIM, HIDDEN), FFN_DIM ** -0.5),
    }


def rms_norm(hidden, gain):
    hidden_f = hidden.astype(jnp.float32)
    variance = jnp.mean(hidden_f * hidden_f, axis=-1, keepdims=True)
    return (hidden_f * lax.rsqrt(variance + 1e-6) * gain.astype(jnp.float32)).astype(jnp.bfloat16)


def rope_tables(positions):
    inv_freq = 1.0 / (1000000.0 ** (jnp.arange(0, HEAD_DIM, 2, dtype=jnp.float32) / HEAD_DIM))
    angles = positions.astype(jnp.float32)[:, None] * inv_freq[None, :]
    return jnp.cos(angles)[:, None, :], jnp.sin(angles)[:, None, :]


def apply_rope(proj_f, cos_tab, sin_tab):
    half_dim = proj_f.shape[-1] // 2
    first_half = proj_f[..., :half_dim]
    second_half = proj_f[..., half_dim:]
    return jnp.concatenate([first_half * cos_tab - second_half * sin_tab, second_half * cos_tab + first_half * sin_tab], axis=-1)


def project(normed, weight, bias_vec):
    return jnp.dot(normed, weight, preferred_element_type=jnp.float32) + bias_vec.astype(jnp.float32)


def attention(queries, key_cache, value_cache, window):
    group_size = Q_HEADS // KV_HEADS
    block_len = 128
    block_count = TOKENS // block_len
    q_blocks = queries.reshape(block_count, block_len, KV_HEADS, group_size, HEAD_DIM).astype(jnp.float32)
    keys_f = key_cache.astype(jnp.float32)
    values_f = value_cache.astype(jnp.float32)
    key_pos = jnp.arange(TOKENS)
    score_scale = HEAD_DIM ** -0.5

    def one_block(block_in):
        block_idx, q_blk = block_in
        query_pos = block_idx * block_len + jnp.arange(block_len)
        scores = jnp.einsum('qkgd,skd->qkgs', q_blk, keys_f) * score_scale
        allowed = (key_pos[None, :] <= query_pos[:, None]) & (key_pos[None, :] > query_pos[:, None] - window)
        scores = jnp.where(allowed[:, None, None, :], scores, -jnp.inf)
        probs = jax.nn.softmax(scores, axis=-1).astype(jnp.bfloat16).astype(jnp.float32)
        return jnp.einsum('qkgs,skd->qkgd', probs, values_f).astype(jnp.bfloat16)

    attn_out = lax.map(one_block, (jnp.arange(block_count), q_blocks))
    return attn_out.reshape(TOKENS, Q_HEADS * HEAD_DIM)


def reference(x_in, positions, attn_gain, mlp_gain, w_query, b_query, w_key, b_key, w_value, b_value, w_out, w_gate, w_up, w_down):
    cos_tab, sin_tab = rope_tables(positions)
    hidden = x_in
    caches = []
    for layer_idx, window in ((0, TOKENS), (1, WINDOW)):
        normed = rms_norm(hidden, attn_gain[layer_idx])
        queries = apply_rope(project(normed, w_query[layer_idx], b_query[layer_idx]).reshape(TOKENS, Q_HEADS, HEAD_DIM), cos_tab, sin_tab).astype(jnp.bfloat16)
        key_cache = apply_rope(project(normed, w_key[layer_idx], b_key[layer_idx]).reshape(TOKENS, KV_HEADS, HEAD_DIM), cos_tab, sin_tab).astype(jnp.bfloat16)
        value_cache = project(normed, w_value[layer_idx], b_value[layer_idx]).astype(jnp.bfloat16).reshape(TOKENS, KV_HEADS, HEAD_DIM)
        attn_out = attention(queries, key_cache, value_cache, window)
        hidden = (hidden.astype(jnp.float32) + jnp.dot(attn_out, w_out[layer_idx], preferred_element_type=jnp.float32)).astype(jnp.bfloat16)
        normed = rms_norm(hidden, mlp_gain[layer_idx])
        gate_proj = jnp.dot(normed, w_gate[layer_idx], preferred_element_type=jnp.float32)
        up_proj = jnp.dot(normed, w_up[layer_idx], preferred_element_type=jnp.float32)
        activated = (jax.nn.silu(gate_proj) * up_proj).astype(jnp.bfloat16)
        hidden = (hidden.astype(jnp.float32) + jnp.dot(activated, w_down[layer_idx], preferred_element_type=jnp.float32)).astype(jnp.bfloat16)
        caches.append(key_cache)
        caches.append(value_cache)
    return (hidden, caches[0], caches[1], caches[2], caches[3])
```

```python
import functools

import jax
import jax.numpy as jnp
from jax import lax
from jax.experimental import pallas as pl
from jax.experimental.pallas import tpu as pltpu
from jax.sharding import PartitionSpec as P

HEAD_DIM = 128
WINDOW = 4096
NEG = -1e37
EXP_SCALE = HEAD_DIM ** -0.5 * 1.4426950408889634


def flash_kernel(n_src, window, bq, bk, chains, fresh, final, deltas, q_ref, *refs):
    kv = refs[:2*n_src]
    refs = refs[2*n_src:]
    if not fresh:
        acc_in, ml_in = refs[:2]; refs=refs[2:]
    if final:
        o_ref=refs[0]; refs=refs[1:]
    else:
        acc_out, ml_out = refs[:2]; refs=refs[2:]
    vts=refs[:n_src]; acc, stat = refs[n_src:]
    i=pl.program_id(1)
    tk=kv[0].shape[0]
    @pl.when(i==0)
    def _():
        for n in range(n_src):
            vts[n][...]=kv[2*n+1][...].T
    if fresh:
        acc[...]=jnp.zeros_like(acc)
        stat[0:1,:]=jnp.full((1,bq),NEG,jnp.float32)
        stat[1:2,:]=jnp.zeros((1,bq),jnp.float32)
    else:
        acc[...]=acc_in[...]
        stat[0:2,:]=ml_in[0,0:2,:]
    t0=i*bq
    cw=bq//chains
    def step(k_ref, vt, delta, j, masked):
        off=pl.multiple_of(j*bk,bk)
        kb=k_ref[pl.ds(off,bk),:]
        vb=vt[:,pl.ds(off,bk)]
        def qk(c):
            return lax.dot_general(kb,q_ref[c*cw:(c+1)*cw,:],(((1,),(1,)),((),())),preferred_element_type=jnp.float32)
        def pv(c,p,alpha):
            sl=slice(c*cw,(c+1)*cw)
            acc[:,sl]=acc[:,sl]*alpha+jnp.dot(vb,p,preferred_element_type=jnp.float32)
        s_next=qk(0)
        pend=None
        for c in range(chains):
            s=s_next; sl=slice(c*cw,(c+1)*cw)
            if c+1<chains: s_next=qk(c+1)
            if pend is not None: pv(*pend)
            if masked:
                rel=lax.broadcasted_iota(jnp.int32,(bk,cw),0)-lax.broadcasted_iota(jnp.int32,(bk,cw),1)+(delta+off-t0-c*cw)
                s=jnp.where((rel<=0)&(rel>-window),s,NEG)
            m_prev=stat[0:1,sl]
            m_new=jnp.maximum(m_prev,jnp.max(s,axis=0,keepdims=True))
            p=jnp.exp2((s-m_new)*EXP_SCALE)
            alpha=jnp.exp2((m_prev-m_new)*EXP_SCALE)
            stat[1:2,sl]=stat[1:2,sl]*alpha+jnp.sum(p,axis=0,keepdims=True)
            stat[0:1,sl]=m_new
            pend=(c,p.astype(jnp.bfloat16),alpha)
        pv(*pend)
    nk=tk//bk
    for n in range(n_src):
        delta=deltas[n]
        hi_any=jnp.clip((t0+bq-1-delta)//bk+1,0,nk)
        hi_full=jnp.clip((t0+1-delta)//bk,0,nk)
        lo_any=jnp.clip((t0-window+1-delta)//bk,0,nk)
        lo_full=jnp.clip((t0+bq-window-delta+bk-1)//bk,0,nk)
        lo_full=jnp.minimum(lo_full,hi_any)
        hi_full=jnp.maximum(hi_full,lo_full)
        def body(masked):
            def f(j,_):
                step(kv[2*n],vts[n],delta,j,masked)
                return 0
            return f
        lax.fori_loop(lo_any,lo_full,body(True),0)
        lax.fori_loop(lo_full,hi_full,body(False),0)
        lax.fori_loop(hi_full,hi_any,body(True),0)
    if final:
        o_ref[...]=(acc[...]*(1.0/stat[1:2,:])).T.astype(o_ref.dtype)
    else:
        acc_out[...]=acc[...]
        ml_out[0,0:2,:]=stat[0:2,:]

def flash(q, sources, deltas, window, first, count, carry=None, final=True, bq=1024, bk=1024, chains=4, units=1.0):
    tq = q.shape[0]
    width = count * HEAD_DIM
    tk = sources[0].shape[0]
    pair = sources[0].shape[1] // (2 * HEAD_DIM)
    n_src = len(sources)
    k_spec = pl.BlockSpec((tk, HEAD_DIM), lambda h, i, d: (0, (first + h) % pair))
    v_spec = pl.BlockSpec((tk, HEAD_DIM), lambda h, i, d: (0, pair + (first + h) % pair))
    in_specs = [pl.BlockSpec((bq, HEAD_DIM), lambda h, i, d: (i, first + h))]
    args = [q]
    for source in sources:
        in_specs += [k_spec, v_spec]
        args += [source, source]
    offset = first % pair
    if carry is not None:
        in_specs += [pl.BlockSpec((HEAD_DIM, bq), lambda h, i, d: (offset + h, i)), pl.BlockSpec((1, 8, bq), lambda h, i, d: (offset + h, 0, i))]
        args += list(carry)
    if final:
        out_shape = jax.ShapeDtypeStruct((tq, width), jnp.bfloat16)
        out_specs = pl.BlockSpec((bq, HEAD_DIM), lambda h, i, d: (i, h))
    else:
        out_shape = (jax.ShapeDtypeStruct((width, tq), jnp.float32), jax.ShapeDtypeStruct((count, 8, tq), jnp.float32))
        out_specs = (pl.BlockSpec((HEAD_DIM, bq), lambda h, i, d: (h, i)), pl.BlockSpec((1, 8, bq), lambda h, i, d: (h, 0, i)))
    return pl.pallas_call(
        functools.partial(flash_kernel, n_src, window, bq, bk, chains, carry is None, final),
        out_shape=out_shape,
        grid_spec=pltpu.PrefetchScalarGridSpec(
            num_scalar_prefetch=1, grid=(count, tq // bq), in_specs=in_specs, out_specs=out_specs,
            scratch_shapes=[pltpu.VMEM((HEAD_DIM, tk), jnp.bfloat16)] * n_src + [pltpu.VMEM((HEAD_DIM, bq), jnp.float32), pltpu.VMEM((8, bq), jnp.float32)]),
        compiler_params=pltpu.CompilerParams(dimension_semantics=("arbitrary", "arbitrary"), vmem_limit_bytes=48 << 20),
        cost_estimate=pl.CostEstimate(flops=int(units * 4 * tq * tk * width), bytes_accessed=8 * tq * width, transcendentals=int(units * tq * tk * count)),
    )(deltas, *args)


def mlp_kernel(tile, first_ref, h_ref, a_ref, b_ref, mine_ref, other_ref, *refs):
    res_ref = refs[0] if len(refs) == 3 else None
    o_ref, acc = refs[-2:]
    step = pl.program_id(0)
    core = first_ref[0]
    half = mine_ref.shape[2]

    @pl.when(step == 0)
    def _():
        if res_ref is None:
            acc[...] = jnp.zeros_like(acc)
        else:
            acc[...] = res_ref[...].astype(jnp.float32)

    across = (((1,), (1,)), ((), ()))
    for r in range(h_ref.shape[0] // tile):
        rows = slice(r * tile, (r + 1) * tile)
        h = h_ref[rows, :]
        a = lax.dot_general(h, a_ref[0], across, preferred_element_type=jnp.float32)
        b = lax.dot_general(h, b_ref[0], across, preferred_element_type=jnp.float32)
        gate = jnp.where(core == 0, a, b)
        up = jnp.where(core == 0, b, a)
        act = (gate * (1.0 / (1.0 + jnp.exp(-gate))) * up).astype(jnp.bfloat16)
        for ref, place in ((mine_ref, core), (other_ref, 1 - core)):
            cols = pl.ds(pl.multiple_of(place * half, half), half)
            acc[rows, cols] += jnp.dot(act, ref[0], preferred_element_type=jnp.float32)

    @pl.when(step == pl.num_programs(0) - 1)
    def _():
        o_ref[...] = acc[...].astype(o_ref.dtype)


def mlp(core, hidden, w_a, w_b, d_mine, d_other, residual=None, tile=256):
    rows, width = hidden.shape
    shards, cols, _ = w_a.shape
    half = d_mine.shape[2]
    out_type = jnp.bfloat16 if residual is None else jnp.float32
    whole = pl.BlockSpec((rows, width), lambda s, c: (0, 0))
    wide = pl.BlockSpec((1, cols, width), lambda s, c: (s, 0, 0))
    down = pl.BlockSpec((1, cols, half), lambda s, c: (s, 0, 0))
    args = [hidden, w_a, w_b, d_mine, d_other] + ([] if residual is None else [residual])
    return pl.pallas_call(
        functools.partial(mlp_kernel, tile),
        out_shape=jax.ShapeDtypeStruct((rows, width), out_type),
        grid_spec=pltpu.PrefetchScalarGridSpec(
            num_scalar_prefetch=1, grid=(shards,),
            in_specs=[whole, wide, wide, down, down] + ([] if residual is None else [whole]),
            out_specs=whole,
            scratch_shapes=[pltpu.VMEM((rows, width), jnp.float32)]),
        compiler_params=pltpu.CompilerParams(dimension_semantics=("arbitrary",), vmem_limit_bytes=56 << 20),
        cost_estimate=pl.CostEstimate(flops=6 * rows * width * cols * shards, bytes_accessed=6 * width * cols * shards, transcendentals=rows * cols * shards),
    )(core, *args)


def select_piece(step, pieces, x_buf):
    whole, halves = pieces[:-2], pieces[-2:]
    for d, ref in enumerate(whole):
        @pl.when(step == d)
        def _():
            x_buf[...] = ref[...]

    @pl.when(step == len(whole))
    def _():
        rows = halves[0].shape[0]
        x_buf[:rows, :] = halves[0][...]
        x_buf[rows:, :] = halves[1][...]


def qkv_kernel(layer, norm, n_pieces, place_ref, *refs):
    pieces, refs = refs[:n_pieces], refs[n_pieces:]
    gain_ref, wq, wk, wv, bq, bk, bv, cos_ref, sin_ref = refs[:9]
    if n_pieces > 1:
        q_ref, kv0_ref, kv1_ref, x_buf = refs[-4:]
        select_piece(pl.program_id(0), pieces, x_buf)
        x = x_buf[...]
    else:
        q_ref, kv0_ref, kv1_ref = refs[-3:]
        x = pieces[0][...]
    if norm:
        xf = x.astype(jnp.float32)
        x = (xf * lax.rsqrt(jnp.mean(xf * xf, axis=-1, keepdims=True) + 1e-6) * gain_ref[layer:layer + 1, :].astype(jnp.float32)).astype(jnp.bfloat16)
    cos, sin = cos_ref[...], sin_ref[...]
    kv = (kv0_ref, kv1_ref)
    width = wq.shape[2]
    pair = kv0_ref.shape[1] // 2
    for w_ref, b_ref, kind in ((wk, bk, 1), (wv, bv, 2), (wq, bq, 0)):
        out = jnp.dot(x, w_ref[0], preferred_element_type=jnp.float32) + b_ref[layer:layer + 1, :].astype(jnp.float32)
        for h in range(width // HEAD_DIM):
            part = out[:, h * HEAD_DIM:(h + 1) * HEAD_DIM]
            if kind != 2:
                part = part * cos + pltpu.roll(part, HEAD_DIM // 2, 1) * sin
            part = part.astype(jnp.bfloat16)
            if kind == 0:
                q_ref[:, h * HEAD_DIM:(h + 1) * HEAD_DIM] = part
            else:
                at = (kind - 1) * pair + (h * HEAD_DIM) % pair
                kv[h * HEAD_DIM // pair][:, at:at + HEAD_DIM] = part


def piece_specs(pieces, steps, tile):
    if len(pieces) == 1:
        return [pl.BlockSpec((tile, pieces[0].shape[1]), lambda i, p: (i, 0))]
    return [pl.BlockSpec(x.shape, lambda i, p: (0, 0)) for x in pieces]


def qkv(layer, norm, place, pieces, gain, weights, biases, cos, sin, block, prior=None, tile=256):
    width = pieces[0].shape[1]
    out_width = weights[0].shape[2]
    steps = place.shape[0]
    spot = lambda i, p: (p[i], 0)
    fixed = lambda shape: pl.BlockSpec(shape, lambda i, p: (0, 0))
    in_specs = piece_specs(pieces, steps, tile) + [fixed(gain.shape)]
    in_specs += [pl.BlockSpec((1, width, out_width), lambda i, p: (layer, 0, 0))] * 3
    in_specs += [fixed(biases[0].shape)] * 3
    in_specs += [pl.BlockSpec((tile, HEAD_DIM), spot)] * 2
    args = [*pieces, gain, *weights, *biases, cos, sin]
    aliases = {}
    if prior is not None:
        aliases = {1 + len(args) + k: k for k in range(3)}
        in_specs += [pl.BlockSpec(memory_space=pl.ANY)] * 3
        args += list(prior)
    return pl.pallas_call(
        functools.partial(qkv_kernel, layer, norm, len(pieces)),
        out_shape=tuple(jax.ShapeDtypeStruct((block, out_width), jnp.bfloat16) for _ in range(3)),
        grid_spec=pltpu.PrefetchScalarGridSpec(
            num_scalar_prefetch=1, grid=(steps,), in_specs=in_specs,
            out_specs=tuple(pl.BlockSpec((tile, out_width), spot) for _ in range(3)),
            scratch_shapes=[pltpu.VMEM((tile, width), jnp.bfloat16)] if len(pieces) > 1 else []),
        input_output_aliases=aliases,
        compiler_params=pltpu.CompilerParams(dimension_semantics=("arbitrary",), vmem_limit_bytes=48 << 20),
        cost_estimate=pl.CostEstimate(flops=6 * steps * tile * width * out_width, bytes_accessed=6 * width * out_width, transcendentals=0),
    )(place, *args)


def put_kernel(n_pieces, place_ref, *refs):
    select_piece(pl.program_id(0), refs[:n_pieces], refs[-1])


def put_rows(place, pieces, block, prior=None):
    tile, width = pieces[0].shape
    steps = place.shape[0]
    args = [*pieces] + ([] if prior is None else [prior])
    return pl.pallas_call(
        functools.partial(put_kernel, len(pieces)),
        out_shape=jax.ShapeDtypeStruct((block, width), pieces[0].dtype),
        grid_spec=pltpu.PrefetchScalarGridSpec(
            num_scalar_prefetch=1, grid=(steps,),
            in_specs=piece_specs(pieces, steps, tile) + ([] if prior is None else [pl.BlockSpec(memory_space=pl.ANY)]),
            out_specs=pl.BlockSpec((tile, width), lambda i, p: (p[i], 0))),
        input_output_aliases={} if prior is None else {1 + len(pieces): 0},
        compiler_params=pltpu.CompilerParams(dimension_semantics=("arbitrary",), vmem_limit_bytes=24 << 20),
        cost_estimate=pl.CostEstimate(flops=10 ** 9, bytes_accessed=4 * steps * tile * width, transcendentals=0),
    )(place, *args)


def normalize(hidden_f, gain):
    variance = jnp.mean(hidden_f * hidden_f, axis=-1, keepdims=True)
    return (hidden_f * lax.rsqrt(variance + 1e-6) * gain.astype(jnp.float32)).astype(jnp.bfloat16)


def rope_tables(positions):
    inv_freq = 1.0 / (1000000.0 ** (jnp.arange(0, HEAD_DIM, 2, dtype=jnp.float32) / HEAD_DIM))
    angles = positions.astype(jnp.float32)[:, None] * inv_freq[None, :]
    cos, sin = jnp.cos(angles), jnp.sin(angles)
    return jnp.concatenate([cos, cos], 1), jnp.concatenate([-sin, sin], 1)


def solution(mesh):
    tp_size = mesh.shape['tp']
    cp_size = mesh.shape['cp']
    swap_x = [(c, c ^ 2) for c in range(cp_size)]
    swap_core = [(c, c ^ 1) for c in range(cp_size)]
    to_later_chip = [(0, 2), (1, 3)]
    to_later_core = [(0, 1), (2, 3)]
    share_late_chip = [(2, 3), (3, 2)]

    def swap_tp(d):
        return [(t, t ^ d) for t in range(tp_size)]

    def local_step(x_in, positions, attn_gain, mlp_gain, w_query, b_query, w_key, b_key, w_value, b_value, w_out, w_gate, w_up, w_down):
        block, width = x_in.shape
        own = block // tp_size
        kv_width = w_key.shape[2]
        pair_width = kv_width // 2
        ffn_half = w_gate.shape[2] // 2
        col_half = width // 2
        t_idx = lax.axis_index('tp').astype(jnp.int32)
        c_idx = lax.axis_index('cp').astype(jnp.int32)
        x_idx = c_idx // 2
        core = c_idx % 2
        core_flag = core.reshape(1)

        def trade(w):
            return lax.ppermute(w, 'cp', swap_core)

        def after(value, *events):
            return lax.optimization_barrier((value,) + events)[0]

        def gather_out(part):
            return lax.all_gather(part, 'tp', axis=0, tiled=True)

        def out_part(layer):
            return lax.dynamic_slice(w_out, (layer, 0, core * col_half), (1, kv_width, col_half))[0]

        def down_part(layer):
            return lax.dynamic_slice(w_down, (layer, x_idx * ffn_half, core * col_half), (1, ffn_half, col_half))[0]

        def wide_part(layer):
            cut = lambda w: lax.dynamic_slice(jnp.swapaxes(w, 1, 2), (layer, x_idx * ffn_half, 0), (1, ffn_half, width))[0]
            return jnp.where(core == 0, cut(w_gate), cut(w_up))

        def gather_stack(part):
            return lax.all_gather(part, 'tp', axis=0)

        def join_cols(mine, other):
            return jnp.where(core == 0, jnp.concatenate([mine, other], 1), jnp.concatenate([other, mine], 1))

        def send_rows(piece, *hold):
            half = piece.shape[0] // 2
            by_y = lax.ppermute(piece, 'tp', swap_tp(1))
            by_z = lax.ppermute(piece, 'tp', swap_tp(2))
            fwd_y, fwd_z = lax.optimization_barrier((by_y, by_z) + hold)[:2] if hold else (by_y, by_z)
            far = (lax.ppermute(fwd_y[:half], 'tp', swap_tp(2)), lax.ppermute(fwd_z[half:], 'tp', swap_tp(1)))
            return (piece, by_y, by_z) + far

        def places(k, chunks):
            return jnp.stack([(t_idx ^ d) * chunks + k for d in range(tp_size)])

        def spread_heads(attn):
            pieces = []
            for d in range(tp_size):
                piece = lax.dynamic_slice_in_dim(attn, (t_idx ^ d) * own, own, 0)
                pieces.append(lax.ppermute(piece, 'tp', swap_tp(d)) if d else piece)
            return pieces

        def collect_heads(groups):
            out = jnp.zeros((own, tp_size * kv_width), jnp.bfloat16)
            for d in range(tp_size):
                piece = jnp.concatenate([g[d] for g in groups], 1)
                out = lax.dynamic_update_slice_in_dim(out, piece, (t_idx ^ d) * kv_width, 1)
            return out

        def delta_of(distance):
            return (((c_idx ^ distance) - c_idx) * block).astype(jnp.int32)

        def attend(queries, packs, window, out_all, wide_all):
            near = jnp.stack([delta_of(0), delta_of(1)])
            far = jnp.stack([delta_of(2), delta_of(3)])
            nearby = [lax.ppermute(p, 'cp', to_later_core) for p in packs]
            remote = [lax.ppermute(p, 'cp', to_later_chip) for p in packs]
            carry = [flash(queries, (packs[g], nearby[g]), near, window, 2 * g, 2, final=False, units=1.5) for g in range(2)]
            far0, carry[1] = lax.optimization_barrier((remote[0], carry[1]))
            sources = (far0, lax.ppermute(far0, 'cp', share_late_chip))
            first = flash(queries, sources, far, window, 0, 1, carry=carry[0], units=2.0)
            far1, first = lax.optimization_barrier((remote[1], first))
            other = (far1, lax.ppermute(far1, 'cp', share_late_chip))
            second = flash(queries, sources, far, window, 1, 1, carry=carry[0], units=2.0)
            sent = spread_heads(jnp.concatenate([first, second], 1))
            rest = flash(queries, other, far, window, 2, 2, carry=carry[1], units=2.0)
            rest, out_all, wide_all = lax.optimization_barrier((rest, out_all, wide_all))
            out_w = (out_all, trade(out_all))
            wide_w = (wide_all, trade(wide_all))
            return collect_heads([sent, spread_heads(rest)]), out_w, wide_w

        cos_tab, sin_tab = rope_tables(positions)
        residual = lax.dynamic_slice_in_dim(x_in, t_idx * own, own, 0).astype(jnp.float32)
        projections = ((w_query, w_key, w_value), (b_query, b_key, b_value))
        out_all = gather_out(out_part(0))
        wide_all = gather_stack(wide_part(0))
        down_all = gather_stack(down_part(0))
        chunks = 2
        piece = own // chunks
        fresh = qkv(0, True, jnp.arange(block // piece, dtype=jnp.int32), (x_in,), attn_gain, *projections, cos_tab, sin_tab, block, tile=piece)
        caches = []
        for layer in range(2):
            window = block * cp_size if layer == 0 else WINDOW
            queries, packs = fresh[0], fresh[1:]
            heads_all, out_w, wide_w = attend(queries, packs, window, out_all, wide_all)
            proj = join_cols(*(jnp.dot(heads_all, w, preferred_element_type=jnp.float32) for w in out_w))
            mid = (residual + proj).astype(jnp.bfloat16)
            h_mid = normalize(mid.astype(jnp.float32), mlp_gain[layer])
            guests = [lax.ppermute(h_mid[k * piece:(k + 1) * piece], 'cp', swap_x) for k in range(chunks)]
            h_mid, down_all = lax.optimization_barrier((h_mid, down_all))
            down_w = (down_all, trade(down_all))
            if layer == 0:
                out_all = gather_out(after(out_part(1), h_mid))
                down_all = gather_stack(after(down_part(1), h_mid))
            mine = mlp(core_flag, h_mid, *wide_w, *down_w, residual=mid)
            guests[0], mine = lax.optimization_barrier((guests[0], mine))
            guest_out = mlp(core_flag, guests[0], *wide_w, *down_w)
            back = [lax.ppermute(guest_out, 'cp', swap_x)]
            guests[1], guest_out = lax.optimization_barrier((guests[1], guest_out))
            guest_last = mlp(core_flag, guests[1], *wide_w, *down_w)
            back.append(lax.ppermute(guest_last, 'cp', swap_x))
            back[0], guest_last = lax.optimization_barrier((back[0], guest_last))
            heads = lambda at: jnp.concatenate([p[:, at:at + pair_width] for p in packs], 1).reshape(block, -1, HEAD_DIM)
            held = [heads(0), heads(pair_width)]
            caches += held
            rest, result, hold = [], None, ()
            for k in range(chunks):
                hidden = (mine[k * piece:(k + 1) * piece] + back[k].astype(jnp.float32)).astype(jnp.bfloat16)
                rest.append(hidden.astype(jnp.float32))
                if layer == 0:
                    pieces = send_rows(normalize(rest[k], attn_gain[1]))
                    result = qkv(1, False, places(k, chunks), pieces, attn_gain, *projections, cos_tab, sin_tab, block, prior=result, tile=piece)
                else:
                    result = put_rows(places(k, chunks), send_rows(hidden), block, result)
            if layer == 0:
                fresh = result
                residual = jnp.concatenate(rest, 0)
                wide_all = gather_stack(after(wide_part(1), fresh[0]))
        return result, caches[0], caches[1], caches[2], caches[3]

    weight_col = P(None, None, 'tp')
    bias_col = P(None, 'tp')
    weight_row = P(None, 'tp', None)
    replicated = P(None, None)
    cache_spec = P('cp', 'tp', None)
    in_specs = (P('cp', None), P('cp'), replicated, replicated, weight_col, bias_col, weight_col, bias_col, weight_col, bias_col, weight_row, weight_col, weight_col, weight_row)
    out_specs = (P('cp', None), cache_spec, cache_spec, cache_spec, cache_spec)
    return jax.shard_map(local_step, mesh=mesh, in_specs=in_specs, out_specs=out_specs, check_vma=False)
```

```python
import functools

import jax
import jax.numpy as jnp
from jax import lax
from jax.experimental import pallas as pl
from jax.experimental.pallas import tpu as pltpu
from jax.sharding import PartitionSpec as P


HEAD_DIM = 128
WINDOW = 4096
NEG = -1e37
EXP_SCALE = HEAD_DIM ** -0.5 * 1.4426950408889634


def flash_kernel(n_src, window, bq, bk, chains, fresh, final, deltas, q_ref, *refs):
    kv = refs[:2 * n_src]
    refs = refs[2 * n_src:]
    if not fresh:
        acc_in, ml_in = refs[:2]
        refs = refs[2:]
    if final:
        o_ref = refs[0]
        refs = refs[1:]
    else:
        acc_out, ml_out = refs[:2]
        refs = refs[2:]
    vts = refs[:n_src]
    acc, stat, s_a, s_b, p_a, p_b = refs[n_src:]
    s_bufs, p_bufs = (s_a, s_b), (p_a, p_b)
    i = pl.program_id(1)
    tk = kv[0].shape[0]

    @pl.when(i == 0)
    def _():
        for n in range(n_src):
            vts[n][...] = kv[2 * n + 1][...].T

    if fresh:
        acc[...] = jnp.zeros_like(acc)
        stat[0:1, :] = jnp.full((1, bq), NEG, jnp.float32)
        stat[1:2, :] = jnp.zeros((1, bq), jnp.float32)
    else:
        acc[...] = acc_in[...]
        stat[0:2, :] = ml_in[0, 0:2, :]
    t0 = i * bq
    cw = bq // chains
    kc, ec = 256, 32
    parts = bk // kc

    def step(k_ref, vt, delta, j, masked):
        off = pl.multiple_of(j * bk, bk)

        def scores(c, r):
            kb = k_ref[pl.ds(off + r * kc, kc), :]
            s = lax.dot_general(kb, q_ref[c * cw:(c + 1) * cw, :], (((1,), (1,)), ((), ())), preferred_element_type=jnp.float32)
            if masked:
                rel = lax.broadcasted_iota(jnp.int32, (kc, cw), 0) - lax.broadcasted_iota(jnp.int32, (kc, cw), 1) + (delta + off + r * kc - t0 - c * cw)
                s = jnp.where((rel <= 0) & (rel > -window), s, NEG)
            s_bufs[c % 2][r * kc:(r + 1) * kc, :] = s
            return jnp.max(s.reshape(kc // 8, 8, cw), axis=0)

        def weigh(c, alpha):
            sl = slice(c * cw, (c + 1) * cw)
            acc[:, sl] = acc[:, sl] * alpha + jnp.dot(vt[:, pl.ds(off, bk)], p_bufs[c % 2][...], preferred_element_type=jnp.float32)

        top = functools.reduce(jnp.maximum, [scores(0, r) for r in range(parts)])
        pending = None
        for c in range(chains):
            sl = slice(c * cw, (c + 1) * cw)
            m_prev = stat[0:1, sl]
            m_new = jnp.maximum(m_prev, jnp.max(top, axis=0, keepdims=True))
            alpha = jnp.exp2((m_prev - m_new) * EXP_SCALE)
            stat[0:1, sl] = m_new
            tops, total = [], None
            for r in range(parts):
                if c + 1 < chains:
                    tops.append(scores(c + 1, r))
                for e in range(r * kc, (r + 1) * kc, ec):
                    p = jnp.exp2((s_bufs[c % 2][e:e + ec, :] - m_new) * EXP_SCALE)
                    p_bufs[c % 2][e:e + ec, :] = p.astype(jnp.bfloat16)
                    part = jnp.sum(p.reshape(ec // 8, 8, cw), axis=0)
                    total = part if total is None else total + part
                if r == 0 and pending is not None:
                    weigh(*pending)
            stat[1:2, sl] = stat[1:2, sl] * alpha + jnp.sum(total, axis=0, keepdims=True)
            pending = (c, alpha)
            if tops:
                top = functools.reduce(jnp.maximum, tops)
        weigh(*pending)

    nk = tk // bk
    for n in range(n_src):
        delta = deltas[n]
        hi_any = jnp.clip((t0 + bq - 1 - delta) // bk + 1, 0, nk)
        hi_full = jnp.clip((t0 + 1 - delta) // bk, 0, nk)
        lo_any = jnp.clip((t0 - window + 1 - delta) // bk, 0, nk)
        lo_full = jnp.clip((t0 + bq - window - delta + bk - 1) // bk, 0, nk)
        lo_full = jnp.minimum(lo_full, hi_any)
        hi_full = jnp.maximum(hi_full, lo_full)

        def body(masked):
            def f(j, _):
                step(kv[2 * n], vts[n], delta, j, masked)
                return 0

            return f

        lax.fori_loop(lo_any, lo_full, body(True), 0)
        lax.fori_loop(lo_full, hi_full, body(False), 0)
        lax.fori_loop(hi_full, hi_any, body(True), 0)
    if final:
        o_ref[...] = (acc[...] * (1.0 / stat[1:2, :])).T.astype(o_ref.dtype)
    else:
        acc_out[...] = acc[...]
        ml_out[0, 0:2, :] = stat[0:2, :]


def flash(q, sources, deltas, window, first, count, carry=None, start=0, final=True, bq=1024, bk=1024, chains=4, units=1.0):
    tq = q.shape[0]
    width = count * HEAD_DIM
    tk = sources[0].shape[0]
    pair = sources[0].shape[1] // (2 * HEAD_DIM)
    n_src = len(sources)
    k_spec = pl.BlockSpec((tk, HEAD_DIM), lambda h, i, d: (0, (first + h) % pair))
    v_spec = pl.BlockSpec((tk, HEAD_DIM), lambda h, i, d: (0, pair + (first + h) % pair))
    in_specs = [pl.BlockSpec((bq, HEAD_DIM), lambda h, i, d: (i, first + h))]
    args = [q]
    for source in sources:
        in_specs += [k_spec, v_spec]
        args += [source, source]
    if carry is not None:
        in_specs += [pl.BlockSpec((HEAD_DIM, bq), lambda h, i, d: (start + h, i)), pl.BlockSpec((1, 8, bq), lambda h, i, d: (start + h, 0, i))]
        args += list(carry)
    if final:
        out_shape = jax.ShapeDtypeStruct((tq, width), jnp.bfloat16)
        out_specs = pl.BlockSpec((bq, HEAD_DIM), lambda h, i, d: (i, h))
    else:
        out_shape = (jax.ShapeDtypeStruct((width, tq), jnp.float32), jax.ShapeDtypeStruct((count, 8, tq), jnp.float32))
        out_specs = (pl.BlockSpec((HEAD_DIM, bq), lambda h, i, d: (h, i)), pl.BlockSpec((1, 8, bq), lambda h, i, d: (h, 0, i)))
    result = pl.pallas_call(
        functools.partial(flash_kernel, n_src, window, bq, bk, chains, carry is None, final),
        out_shape=out_shape,
        grid_spec=pltpu.PrefetchScalarGridSpec(
            num_scalar_prefetch=1, grid=(count, tq // bq), in_specs=in_specs, out_specs=out_specs,
            scratch_shapes=[pltpu.VMEM((HEAD_DIM, tk), jnp.bfloat16)] * n_src + [pltpu.VMEM((HEAD_DIM, bq), jnp.float32), pltpu.VMEM((8, bq), jnp.float32)]
            + [pltpu.VMEM((bk, bq // chains), jnp.float32)] * 2 + [pltpu.VMEM((bk, bq // chains), jnp.bfloat16)] * 2),
        compiler_params=pltpu.CompilerParams(dimension_semantics=("arbitrary", "arbitrary"), vmem_limit_bytes=48 << 20),
        cost_estimate=pl.CostEstimate(flops=int(units * 4 * tq * tk * width), bytes_accessed=8 * tq * width, transcendentals=int(units * tq * tk * count)),
    )(deltas, *args)
    return result if final else list(result)


def mlp_kernel(tile, first_ref, h_ref, a_ref, b_ref, mine_ref, other_ref, *refs):
    res_ref = refs[0] if len(refs) == 3 else None
    o_ref, acc = refs[-2:]
    step = pl.program_id(0)
    core = first_ref[0]
    half = mine_ref.shape[2]

    @pl.when(step == 0)
    def _():
        if res_ref is None:
            acc[...] = jnp.zeros_like(acc)
        else:
            acc[...] = res_ref[...].astype(jnp.float32)

    across = (((1,), (1,)), ((), ()))
    for r in range(h_ref.shape[0] // tile):
        rows = slice(r * tile, (r + 1) * tile)
        h = h_ref[rows, :]
        a = lax.dot_general(h, a_ref[0], across, preferred_element_type=jnp.float32)
        b = lax.dot_general(h, b_ref[0], across, preferred_element_type=jnp.float32)
        gate = jnp.where(core == 0, a, b)
        up = jnp.where(core == 0, b, a)
        act = (gate * (1.0 / (1.0 + jnp.exp(-gate))) * up).astype(jnp.bfloat16)
        for ref, place in ((mine_ref, core), (other_ref, 1 - core)):
            cols = pl.ds(pl.multiple_of(place * half, half), half)
            acc[rows, cols] += jnp.dot(act, ref[0], preferred_element_type=jnp.float32)

    @pl.when(step == pl.num_programs(0) - 1)
    def _():
        o_ref[...] = acc[...].astype(o_ref.dtype)


def mlp(core, hidden, w_a, w_b, d_mine, d_other, residual=None, tile=256):
    rows, width = hidden.shape
    shards, cols, _ = w_a.shape
    half = d_mine.shape[2]
    out_type = jnp.bfloat16 if residual is None else jnp.float32
    whole = pl.BlockSpec((rows, width), lambda s, c: (0, 0))
    wide = pl.BlockSpec((1, cols, width), lambda s, c: (s, 0, 0))
    down = pl.BlockSpec((1, cols, half), lambda s, c: (s, 0, 0))
    args = [hidden, w_a, w_b, d_mine, d_other] + ([] if residual is None else [residual])
    return pl.pallas_call(
        functools.partial(mlp_kernel, min(tile, rows)),
        out_shape=jax.ShapeDtypeStruct((rows, width), out_type),
        grid_spec=pltpu.PrefetchScalarGridSpec(
            num_scalar_prefetch=1, grid=(shards,),
            in_specs=[whole, wide, wide, down, down] + ([] if residual is None else [whole]),
            out_specs=whole,
            scratch_shapes=[pltpu.VMEM((rows, width), jnp.float32)]),
        compiler_params=pltpu.CompilerParams(dimension_semantics=("arbitrary",), vmem_limit_bytes=56 << 20),
        cost_estimate=pl.CostEstimate(flops=6 * rows * width * cols * shards, bytes_accessed=6 * width * cols * shards, transcendentals=rows * cols * shards),
    )(core, *args)


def select_piece(step, pieces, x_buf):
    whole, halves = pieces[:-2], pieces[-2:]
    for d, ref in enumerate(whole):
        @pl.when(step == d)
        def _():
            x_buf[...] = ref[...]

    @pl.when(step == len(whole))
    def _():
        rows = halves[0].shape[0]
        x_buf[:rows, :] = halves[0][...]
        x_buf[rows:, :] = halves[1][...]


def qkv_kernel(layer, norm, n_pieces, place_ref, *refs):
    pieces, refs = refs[:n_pieces], refs[n_pieces:]
    gain_ref, wq, wk, wv, bq, bk, bv, cos_ref, sin_ref = refs[:9]
    if n_pieces > 1:
        q_ref, kv0_ref, kv1_ref, x_buf = refs[-4:]
        select_piece(pl.program_id(0), pieces, x_buf)
        x = x_buf[...]
    else:
        q_ref, kv0_ref, kv1_ref = refs[-3:]
        x = pieces[0][...]
    if norm:
        xf = x.astype(jnp.float32)
        x = (xf * lax.rsqrt(jnp.mean(xf * xf, axis=-1, keepdims=True) + 1e-6) * gain_ref[layer:layer + 1, :].astype(jnp.float32)).astype(jnp.bfloat16)
    cos, sin = cos_ref[...], sin_ref[...]
    kv = (kv0_ref, kv1_ref)
    width = wq.shape[2]
    pair = kv0_ref.shape[1] // 2
    for w_ref, b_ref, kind in ((wk, bk, 1), (wv, bv, 2), (wq, bq, 0)):
        out = jnp.dot(x, w_ref[0], preferred_element_type=jnp.float32) + b_ref[layer:layer + 1, :].astype(jnp.float32)
        for h in range(width // HEAD_DIM):
            part = out[:, h * HEAD_DIM:(h + 1) * HEAD_DIM]
            if kind != 2:
                part = part * cos + pltpu.roll(part, HEAD_DIM // 2, 1) * sin
            part = part.astype(jnp.bfloat16)
            if kind == 0:
                q_ref[:, h * HEAD_DIM:(h + 1) * HEAD_DIM] = part
            else:
                at = (kind - 1) * pair + (h * HEAD_DIM) % pair
                kv[h * HEAD_DIM // pair][:, at:at + HEAD_DIM] = part


def piece_specs(pieces, tile):
    if len(pieces) == 1:
        return [pl.BlockSpec((tile, pieces[0].shape[1]), lambda i, p: (i, 0))]
    return [pl.BlockSpec(x.shape, lambda i, p: (0, 0)) for x in pieces]


def qkv(layer, norm, place, pieces, gain, weights, biases, cos, sin, block, prior=None, tile=256):
    width = pieces[0].shape[1]
    out_width = weights[0].shape[2]
    steps = place.shape[0]
    spot = lambda i, p: (p[i], 0)
    fixed = lambda shape: pl.BlockSpec(shape, lambda i, p: (0, 0))
    in_specs = piece_specs(pieces, tile) + [fixed(gain.shape)]
    in_specs += [pl.BlockSpec((1, width, out_width), lambda i, p: (layer, 0, 0))] * 3
    in_specs += [fixed(biases[0].shape)] * 3
    in_specs += [pl.BlockSpec((tile, HEAD_DIM), spot)] * 2
    args = [*pieces, gain, *weights, *biases, cos, sin]
    aliases = {}
    if prior is not None:
        aliases = {1 + len(args) + k: k for k in range(3)}
        in_specs += [pl.BlockSpec(memory_space=pl.ANY)] * 3
        args += list(prior)
    return pl.pallas_call(
        functools.partial(qkv_kernel, layer, norm, len(pieces)),
        out_shape=tuple(jax.ShapeDtypeStruct((block, out_width), jnp.bfloat16) for _ in range(3)),
        grid_spec=pltpu.PrefetchScalarGridSpec(
            num_scalar_prefetch=1, grid=(steps,), in_specs=in_specs,
            out_specs=tuple(pl.BlockSpec((tile, out_width), spot) for _ in range(3)),
            scratch_shapes=[pltpu.VMEM((tile, width), jnp.bfloat16)] if len(pieces) > 1 else []),
        input_output_aliases=aliases,
        compiler_params=pltpu.CompilerParams(dimension_semantics=("arbitrary",), vmem_limit_bytes=48 << 20),
        cost_estimate=pl.CostEstimate(flops=6 * steps * tile * width * out_width, bytes_accessed=6 * width * out_width, transcendentals=0),
    )(place, *args)


def put_kernel(n_pieces, place_ref, *refs):
    select_piece(pl.program_id(0), refs[:n_pieces], refs[-1])


def put_rows(place, pieces, block, prior=None):
    tile, width = pieces[0].shape
    steps = place.shape[0]
    args = [*pieces] + ([] if prior is None else [prior])
    return pl.pallas_call(
        functools.partial(put_kernel, len(pieces)),
        out_shape=jax.ShapeDtypeStruct((block, width), pieces[0].dtype),
        grid_spec=pltpu.PrefetchScalarGridSpec(
            num_scalar_prefetch=1, grid=(steps,),
            in_specs=piece_specs(pieces, tile) + ([] if prior is None else [pl.BlockSpec(memory_space=pl.ANY)]),
            out_specs=pl.BlockSpec((tile, width), lambda i, p: (p[i], 0))),
        input_output_aliases={} if prior is None else {1 + len(pieces): 0},
        compiler_params=pltpu.CompilerParams(dimension_semantics=("arbitrary",), vmem_limit_bytes=24 << 20),
        cost_estimate=pl.CostEstimate(flops=10 ** 9, bytes_accessed=4 * steps * tile * width, transcendentals=0),
    )(place, *args)


def normalize(hidden_f, gain):
    variance = jnp.mean(hidden_f * hidden_f, axis=-1, keepdims=True)
    return (hidden_f * lax.rsqrt(variance + 1e-6) * gain.astype(jnp.float32)).astype(jnp.bfloat16)


def rope_tables(positions):
    inv_freq = 1.0 / (1000000.0 ** (jnp.arange(0, HEAD_DIM, 2, dtype=jnp.float32) / HEAD_DIM))
    angles = positions.astype(jnp.float32)[:, None] * inv_freq[None, :]
    cos, sin = jnp.cos(angles), jnp.sin(angles)
    return jnp.concatenate([cos, cos], 1), jnp.concatenate([-sin, sin], 1)


def solution(mesh):
    tp_size = mesh.shape['tp']
    cp_size = mesh.shape['cp']
    swap_x = [(c, c ^ 2) for c in range(cp_size)]
    swap_core = [(c, c ^ 1) for c in range(cp_size)]
    to_later_chip = [(0, 2), (1, 3)]
    to_later_core = [(0, 1), (2, 3)]
    share_late_chip = [(2, 3), (3, 2)]

    def swap_tp(d):
        return [(t, t ^ d) for t in range(tp_size)]

    def local_step(x_in, positions, attn_gain, mlp_gain, w_query, b_query, w_key, b_key, w_value, b_value, w_out, w_gate, w_up, w_down):
        block, width = x_in.shape
        own = block // tp_size
        kv_width = w_key.shape[2]
        pair_width = kv_width // 2
        ffn_half = w_gate.shape[2] // 2
        col_half = width // 2
        t_idx = lax.axis_index('tp').astype(jnp.int32)
        c_idx = lax.axis_index('cp').astype(jnp.int32)
        x_idx = c_idx // 2
        core = c_idx % 2
        core_flag = core.reshape(1)

        def trade(w):
            return lax.ppermute(w, 'cp', swap_core)

        def after(value, *events):
            return lax.optimization_barrier((value,) + events)[0]

        def gather_out(part):
            return lax.all_gather(part, 'tp', axis=0, tiled=True)

        def out_part(layer):
            return lax.dynamic_slice(w_out, (layer, 0, core * col_half), (1, kv_width, col_half))[0]

        def down_part(layer):
            return lax.dynamic_slice(w_down, (layer, x_idx * ffn_half, core * col_half), (1, ffn_half, col_half))[0]

        def wide_part(layer, *events):
            w_gate_l, w_up_l = lax.optimization_barrier((w_gate, w_up) + events)[:2]
            cut = lambda w: lax.dynamic_slice(jnp.swapaxes(w, 1, 2), (layer, x_idx * ffn_half, 0), (1, ffn_half, width))[0]
            return jnp.where(core == 0, cut(w_gate_l), cut(w_up_l))

        def gather_stack(part):
            return lax.all_gather(part, 'tp', axis=0)

        def join_cols(mine, other):
            return jnp.where(core == 0, jnp.concatenate([mine, other], 1), jnp.concatenate([other, mine], 1))

        def places(k, chunks):
            return jnp.stack([(t_idx ^ d) * chunks + k for d in range(tp_size)])

        def spread_heads(attn):
            pieces = []
            for d in range(tp_size):
                piece = lax.dynamic_slice_in_dim(attn, (t_idx ^ d) * own, own, 0)
                pieces.append(lax.ppermute(piece, 'tp', swap_tp(d)) if d else piece)
            return pieces

        def collect_heads(groups):
            return jnp.concatenate([g[d] for d in range(tp_size) for g in groups], 1)

        def by_distance(gathered):
            return jnp.concatenate([lax.dynamic_slice_in_dim(gathered, (t_idx ^ d) * kv_width, kv_width, 0) for d in range(tp_size)], 0)

        def delta_of(distance):
            return (((c_idx ^ distance) - c_idx) * block).astype(jnp.int32)

        def attend(queries, packs, window, out_all, wide_all):
            near = jnp.stack([delta_of(0), delta_of(1)])
            far = jnp.stack([delta_of(2), delta_of(3)])
            nearby = [lax.ppermute(p, 'cp', to_later_core) for p in packs]
            remote = []
            for pack in packs:
                remote.append(lax.ppermute(pack, 'cp', to_later_chip))

            def local(g, first, count, held):
                return flash(held, (packs[g], nearby[g]), near, window, first, count, final=False, units=1.5)

            both = local(0, 0, 2, queries)
            held, both[1] = lax.optimization_barrier((queries, both[1]))
            third = local(1, 2, 1, held)
            held, third[1], far0 = lax.optimization_barrier((held, third[1], remote[0]))
            sources = (far0, lax.ppermute(far0, 'cp', share_late_chip))
            fourth = local(1, 3, 1, held)

            def finish(head, carry, start, held):
                return flash(held, sources if head < 2 else other, far, window, head, 1, carry=carry, start=start, units=2.0)

            held, fourth[1] = lax.optimization_barrier((held, fourth[1]))
            outs = [finish(0, both, 0, held)]
            far1, held, outs[0] = lax.optimization_barrier((remote[1], held, outs[0]))
            other = (far1, lax.ppermute(far1, 'cp', share_late_chip))
            sent = [spread_heads(outs[0])]
            outs.append(finish(1, both, 1, held))
            held, outs[1] = lax.optimization_barrier((held, outs[1]))
            sent.append(spread_heads(outs[1]))
            outs.append(finish(2, third, 0, held))
            held, outs[2], out_all, wide_all = lax.optimization_barrier((held, outs[2], out_all, wide_all))
            out_w = (out_all, trade(out_all))
            wide_w = (wide_all, trade(wide_all))
            sent.append(spread_heads(outs[2]))
            sent.append(spread_heads(finish(3, fourth, 0, held)))
            return collect_heads(sent), out_w, wide_w

        cos_tab, sin_tab = rope_tables(positions)
        residual = lax.dynamic_slice_in_dim(x_in, t_idx * own, own, 0).astype(jnp.float32)
        projections = ((w_query, w_key, w_value), (b_query, b_key, b_value))
        out_all = by_distance(gather_out(out_part(0)))
        chunks = 2
        piece = own // chunks
        fresh = qkv(0, True, jnp.arange(block // piece, dtype=jnp.int32), (x_in,), attn_gain, *projections, cos_tab, sin_tab, block, tile=piece)
        wide_all = gather_stack(wide_part(0, fresh[0]))
        down_all = gather_stack(after(down_part(0), fresh[0]))
        caches = []
        for layer in range(2):
            window = block * cp_size if layer == 0 else WINDOW
            queries, packs = fresh[0], fresh[1:]
            heads_all, out_w, wide_w = attend(queries, packs, window, out_all, wide_all)
            proj = join_cols(*(jnp.dot(heads_all, w, preferred_element_type=jnp.float32) for w in out_w))
            mid = (residual + proj).astype(jnp.bfloat16)
            h_mid = normalize(mid.astype(jnp.float32), mlp_gain[layer])
            guests = [lax.ppermute(h_mid[k * piece:(k + 1) * piece], 'cp', swap_x) for k in range(chunks)]
            h_mid, down_all = lax.optimization_barrier((h_mid, down_all))
            down_w = (down_all, trade(down_all))
            if layer == 0:
                out_all = by_distance(gather_out(after(out_part(1), h_mid)))
                down_all = gather_stack(after(down_part(1), h_mid))
            mine = mlp(core_flag, h_mid, *wide_w, *down_w, residual=mid)
            guests[0], mine = lax.optimization_barrier((guests[0], mine))
            guest_out = mlp(core_flag, guests[0], *wide_w, *down_w)
            back = [lax.ppermute(guest_out, 'cp', swap_x)]
            guests[1], guest_out = lax.optimization_barrier((guests[1], guest_out))
            guest_last = mlp(core_flag, guests[1], *wide_w, *down_w)
            back.append(lax.ppermute(guest_last, 'cp', swap_x))
            back[0], guest_last = lax.optimization_barrier((back[0], guest_last))
            heads = lambda at: jnp.concatenate([p[:, at:at + pair_width] for p in packs], 1).reshape(block, -1, HEAD_DIM)
            held = [heads(0), heads(pair_width)]
            caches += held
            rest, result, last = [], None, back[1]
            if layer == 0:
                wide_next, last = lax.optimization_barrier((wide_part(1, guest_last), last))
            for k in range(chunks):
                from_guest = back[0] if k == 0 else last
                hidden = (mine[k * piece:(k + 1) * piece] + from_guest.astype(jnp.float32)).astype(jnp.bfloat16)
                rest.append(hidden.astype(jnp.float32))
                rows = normalize(rest[k], attn_gain[1]) if layer == 0 else hidden
                by_y = lax.ppermute(rows, 'tp', swap_tp(1))
                by_z = lax.ppermute(rows, 'tp', swap_tp(2))
                if k == 0:
                    by_y, by_z, last = lax.optimization_barrier((by_y, by_z, last))
                elif layer == 0:
                    by_y, by_z, result[0] = lax.optimization_barrier((by_y, by_z, result[0]))
                else:
                    by_y, by_z, result = lax.optimization_barrier((by_y, by_z, result))
                half = piece // 2
                pieces = (rows, by_y, by_z, lax.ppermute(by_y[:half], 'tp', swap_tp(2)), lax.ppermute(by_z[half:], 'tp', swap_tp(1)))
                if layer == 0:
                    result = list(qkv(1, False, places(k, chunks), pieces, attn_gain, *projections, cos_tab, sin_tab, block, prior=result, tile=piece))
                else:
                    result = put_rows(places(k, chunks), pieces, block, result)
            if layer == 0:
                fresh = result
                residual = jnp.concatenate(rest, 0)
                wide_all = gather_stack(after(wide_next, fresh[0], down_all))
        return result, caches[0], caches[1], caches[2], caches[3]

    weight_col = P(None, None, 'tp')
    bias_col = P(None, 'tp')
    weight_row = P(None, 'tp', None)
    replicated = P(None, None)
    cache_spec = P('cp', 'tp', None)
    in_specs = (P('cp', None), P('cp'), replicated, replicated, weight_col, bias_col, weight_col, bias_col, weight_col, bias_col, weight_row, weight_col, weight_col, weight_row)
    out_specs = (P('cp', None), cache_spec, cache_spec, cache_spec, cache_spec)
    return jax.shard_map(local_step, mesh=mesh, in_specs=in_specs, out_specs=out_specs, check_vma=False)
```

```python
import functools

import jax
import jax.numpy as jnp
from jax import lax
from jax.experimental import pallas as pl
from jax.experimental.pallas import tpu as pltpu
from jax.sharding import PartitionSpec as P


HEAD_DIM = 128
WINDOW = 4096
NEG = -1e37
EXP_SCALE = HEAD_DIM ** -0.5 * 1.4426950408889634


def flash_kernel(n_src, window, bq, bk, chains, fresh, final, deltas, q_ref, *refs):
    kv = refs[:2 * n_src]
    refs = refs[2 * n_src:]
    if not fresh:
        acc_in, ml_in = refs[:2]
        refs = refs[2:]
    if final:
        o_ref = refs[0]
        refs = refs[1:]
    else:
        acc_out, ml_out = refs[:2]
        refs = refs[2:]
    vts = refs[:n_src]
    acc, stat, s_a, s_b, p_a, p_b = refs[n_src:]
    s_bufs, p_bufs = (s_a, s_b), (p_a, p_b)
    i = pl.program_id(1)
    tk = kv[0].shape[0]

    @pl.when(i == 0)
    def _():
        for n in range(n_src):
            vts[n][...] = kv[2 * n + 1][...].T

    if fresh:
        acc[...] = jnp.zeros_like(acc)
        stat[0:1, :] = jnp.full((1, bq), NEG, jnp.float32)
        stat[1:2, :] = jnp.zeros((1, bq), jnp.float32)
    else:
        acc[...] = acc_in[...]
        stat[0:2, :] = ml_in[0, 0:2, :]
    t0 = i * bq
    cw = bq // chains
    kc, ec = 256, 32
    parts = bk // kc
    assert bq == bk and cw == kc and window % bk == 0

    def step(k_ref, vt, j, edge):
        off = pl.multiple_of(j * bk, bk)

        def span(c):
            if edge == 'causal':
                return range(c + 1)
            return range(c, parts) if edge == 'window' else range(parts)

        def scores(c, r):
            kb = k_ref[pl.ds(off + r * kc, kc), :]
            s = lax.dot_general(kb, q_ref[c * cw:(c + 1) * cw, :], (((1,), (1,)), ((), ())), preferred_element_type=jnp.float32)
            if edge and r == c:
                key_at, query_at = (lax.broadcasted_iota(jnp.int32, (kc, cw), axis) for axis in range(2))
                s = jnp.where(key_at <= query_at if edge == 'causal' else key_at > query_at, s, NEG)
            s_bufs[c % 2][r * kc:(r + 1) * kc, :] = s
            return jnp.max(s.reshape(kc // 8, 8, cw), axis=0)

        def weigh(c, alpha):
            sl = slice(c * cw, (c + 1) * cw)
            lo, hi = span(c)[0] * kc, (span(c)[-1] + 1) * kc
            acc[:, sl] = acc[:, sl] * alpha + jnp.dot(vt[:, pl.ds(off + lo, hi - lo)], p_bufs[c % 2][lo:hi, :], preferred_element_type=jnp.float32)

        top = functools.reduce(jnp.maximum, [scores(0, r) for r in span(0)])
        pending = None
        for c in range(chains):
            sl = slice(c * cw, (c + 1) * cw)
            m_prev = stat[0:1, sl]
            m_new = jnp.maximum(m_prev, jnp.max(top, axis=0, keepdims=True))
            alpha = jnp.exp2((m_prev - m_new) * EXP_SCALE)
            stat[0:1, sl] = m_new
            following = list(span(c + 1)) if c + 1 < chains else []
            tops, total = [], None
            for n in range(parts):
                if n < len(following):
                    tops.append(scores(c + 1, following[n]))
                if n < len(span(c)):
                    r = span(c)[n]
                    for e in range(r * kc, (r + 1) * kc, ec):
                        p = jnp.exp2((s_bufs[c % 2][e:e + ec, :] - m_new) * EXP_SCALE)
                        p_bufs[c % 2][e:e + ec, :] = p.astype(jnp.bfloat16)
                        part = jnp.sum(p.reshape(ec // 8, 8, cw), axis=0)
                        total = part if total is None else total + part
                if n == 0 and pending is not None:
                    weigh(*pending)
            stat[1:2, sl] = stat[1:2, sl] * alpha + jnp.sum(total, axis=0, keepdims=True)
            pending = (c, alpha)
            if tops:
                top = functools.reduce(jnp.maximum, tops)
        weigh(*pending)

    nk = tk // bk
    for n in range(n_src):
        delta = deltas[n]
        hi_any = jnp.clip((t0 + bq - 1 - delta) // bk + 1, 0, nk)
        hi_full = jnp.clip((t0 + 1 - delta) // bk, 0, nk)
        lo_any = jnp.clip((t0 - window + 1 - delta) // bk, 0, nk)
        lo_full = jnp.clip((t0 + bq - window - delta + bk - 1) // bk, 0, nk)
        lo_full = jnp.minimum(lo_full, hi_any)
        hi_full = jnp.maximum(hi_full, lo_full)

        def body(edge):
            def f(j, _):
                step(kv[2 * n], vts[n], j, edge)
                return 0

            return f

        lax.fori_loop(lo_any, lo_full, body('window'), 0)
        lax.fori_loop(lo_full, hi_full, body(None), 0)
        lax.fori_loop(hi_full, hi_any, body('causal'), 0)
    if final:
        o_ref[...] = (acc[...] * (1.0 / stat[1:2, :])).T.astype(o_ref.dtype)
    else:
        acc_out[...] = acc[...]
        ml_out[0, 0:2, :] = stat[0:2, :]


def flash(q, sources, deltas, window, first, count, carry=None, start=0, final=True, bq=1024, bk=1024, chains=4, units=1.0):
    tq = q.shape[0]
    width = count * HEAD_DIM
    tk = sources[0].shape[0]
    pair = sources[0].shape[1] // (2 * HEAD_DIM)
    n_src = len(sources)
    k_spec = pl.BlockSpec((tk, HEAD_DIM), lambda h, i, d: (0, (first + h) % pair))
    v_spec = pl.BlockSpec((tk, HEAD_DIM), lambda h, i, d: (0, pair + (first + h) % pair))
    in_specs = [pl.BlockSpec((bq, HEAD_DIM), lambda h, i, d: (i, first + h))]
    args = [q]
    for source in sources:
        in_specs += [k_spec, v_spec]
        args += [source, source]
    if carry is not None:
        in_specs += [pl.BlockSpec((HEAD_DIM, bq), lambda h, i, d: (start + h, i)), pl.BlockSpec((1, 8, bq), lambda h, i, d: (start + h, 0, i))]
        args += list(carry)
    if final:
        out_shape = jax.ShapeDtypeStruct((tq, width), jnp.bfloat16)
        out_specs = pl.BlockSpec((bq, HEAD_DIM), lambda h, i, d: (i, h))
    else:
        out_shape = (jax.ShapeDtypeStruct((width, tq), jnp.float32), jax.ShapeDtypeStruct((count, 8, tq), jnp.float32))
        out_specs = (pl.BlockSpec((HEAD_DIM, bq), lambda h, i, d: (h, i)), pl.BlockSpec((1, 8, bq), lambda h, i, d: (h, 0, i)))
    result = pl.pallas_call(
        functools.partial(flash_kernel, n_src, window, bq, bk, chains, carry is None, final),
        out_shape=out_shape,
        grid_spec=pltpu.PrefetchScalarGridSpec(
            num_scalar_prefetch=1, grid=(count, tq // bq), in_specs=in_specs, out_specs=out_specs,
            scratch_shapes=[pltpu.VMEM((HEAD_DIM, tk), jnp.bfloat16)] * n_src + [pltpu.VMEM((HEAD_DIM, bq), jnp.float32), pltpu.VMEM((8, bq), jnp.float32)]
            + [pltpu.VMEM((bk, bq // chains), jnp.float32)] * 2 + [pltpu.VMEM((bk, bq // chains), jnp.bfloat16)] * 2),
        compiler_params=pltpu.CompilerParams(dimension_semantics=("arbitrary", "arbitrary"), vmem_limit_bytes=48 << 20),
        cost_estimate=pl.CostEstimate(flops=int(units * 4 * tq * tk * width), bytes_accessed=8 * tq * width, transcendentals=int(units * tq * tk * count)),
    )(deltas, *args)
    return result if final else list(result)


def mlp_kernel(tile, first_ref, h_ref, a_ref, b_ref, mine_ref, other_ref, *refs):
    res_ref = refs[0] if len(refs) == 3 else None
    o_ref, acc = refs[-2:]
    step = pl.program_id(0)
    core = first_ref[0]
    half = mine_ref.shape[2]

    @pl.when(step == 0)
    def _():
        if res_ref is None:
            acc[...] = jnp.zeros_like(acc)
        else:
            acc[...] = res_ref[...].astype(jnp.float32)

    across = (((1,), (1,)), ((), ()))
    for r in range(h_ref.shape[0] // tile):
        rows = slice(r * tile, (r + 1) * tile)
        h = h_ref[rows, :]
        a = lax.dot_general(h, a_ref[0], across, preferred_element_type=jnp.float32)
        b = lax.dot_general(h, b_ref[0], across, preferred_element_type=jnp.float32)
        gate = jnp.where(core == 0, a, b)
        up = jnp.where(core == 0, b, a)
        act = (gate * (1.0 / (1.0 + jnp.exp(-gate))) * up).astype(jnp.bfloat16)
        for ref, place in ((mine_ref, core), (other_ref, 1 - core)):
            cols = pl.ds(pl.multiple_of(place * half, half), half)
            acc[rows, cols] += jnp.dot(act, ref[0], preferred_element_type=jnp.float32)

    @pl.when(step == pl.num_programs(0) - 1)
    def _():
        o_ref[...] = acc[...].astype(o_ref.dtype)


def mlp(core, hidden, w_a, w_b, d_mine, d_other, residual=None, tile=256):
    rows, width = hidden.shape
    shards, cols, _ = w_a.shape
    half = d_mine.shape[2]
    out_type = jnp.bfloat16 if residual is None else jnp.float32
    whole = pl.BlockSpec((rows, width), lambda s, c: (0, 0))
    wide = pl.BlockSpec((1, cols, width), lambda s, c: (s, 0, 0))
    down = pl.BlockSpec((1, cols, half), lambda s, c: (s, 0, 0))
    args = [hidden, w_a, w_b, d_mine, d_other] + ([] if residual is None else [residual])
    return pl.pallas_call(
        functools.partial(mlp_kernel, min(tile, rows)),
        out_shape=jax.ShapeDtypeStruct((rows, width), out_type),
        grid_spec=pltpu.PrefetchScalarGridSpec(
            num_scalar_prefetch=1, grid=(shards,),
            in_specs=[whole, wide, wide, down, down] + ([] if residual is None else [whole]),
            out_specs=whole,
            scratch_shapes=[pltpu.VMEM((rows, width), jnp.float32)]),
        compiler_params=pltpu.CompilerParams(dimension_semantics=("arbitrary",), vmem_limit_bytes=56 << 20),
        cost_estimate=pl.CostEstimate(flops=6 * rows * width * cols * shards, bytes_accessed=6 * width * cols * shards, transcendentals=rows * cols * shards),
    )(core, *args)


def select_piece(step, pieces, x_buf):
    whole, halves = pieces[:-2], pieces[-2:]
    for d, ref in enumerate(whole):
        @pl.when(step == d)
        def _():
            x_buf[...] = ref[...]

    @pl.when(step == len(whole))
    def _():
        rows = halves[0].shape[0]
        x_buf[:rows, :] = halves[0][...]
        x_buf[rows:, :] = halves[1][...]


def qkv_kernel(layer, norm, n_pieces, place_ref, *refs):
    pieces, refs = refs[:n_pieces], refs[n_pieces:]
    gain_ref, wq, wk, wv, bq, bk, bv, cos_ref, sin_ref = refs[:9]
    if n_pieces > 1:
        q_ref, kv0_ref, kv1_ref, x_buf = refs[-4:]
        select_piece(pl.program_id(0), pieces, x_buf)
        x = x_buf[...]
    else:
        q_ref, kv0_ref, kv1_ref = refs[-3:]
        x = pieces[0][...]
    if norm:
        xf = x.astype(jnp.float32)
        x = (xf * lax.rsqrt(jnp.mean(xf * xf, axis=-1, keepdims=True) + 1e-6) * gain_ref[layer:layer + 1, :].astype(jnp.float32)).astype(jnp.bfloat16)
    cos, sin = cos_ref[...], sin_ref[...]
    kv = (kv0_ref, kv1_ref)
    width = wq.shape[2]
    pair = kv0_ref.shape[1] // 2
    for w_ref, b_ref, kind in ((wk, bk, 1), (wv, bv, 2), (wq, bq, 0)):
        out = jnp.dot(x, w_ref[0], preferred_element_type=jnp.float32) + b_ref[layer:layer + 1, :].astype(jnp.float32)
        for h in range(width // HEAD_DIM):
            part = out[:, h * HEAD_DIM:(h + 1) * HEAD_DIM]
            if kind != 2:
                part = part * cos + pltpu.roll(part, HEAD_DIM // 2, 1) * sin
            part = part.astype(jnp.bfloat16)
            if kind == 0:
                q_ref[:, h * HEAD_DIM:(h + 1) * HEAD_DIM] = part
            else:
                at = (kind - 1) * pair + (h * HEAD_DIM) % pair
                kv[h * HEAD_DIM // pair][:, at:at + HEAD_DIM] = part


def piece_specs(pieces, tile):
    if len(pieces) == 1:
        return [pl.BlockSpec((tile, pieces[0].shape[1]), lambda i, p: (i, 0))]
    return [pl.BlockSpec(x.shape, lambda i, p: (0, 0)) for x in pieces]


def qkv(layer, norm, place, pieces, gain, weights, biases, cos, sin, block, prior=None, tile=256):
    width = pieces[0].shape[1]
    out_width = weights[0].shape[2]
    steps = place.shape[0]
    spot = lambda i, p: (p[i], 0)
    fixed = lambda shape: pl.BlockSpec(shape, lambda i, p: (0, 0))
    in_specs = piece_specs(pieces, tile) + [fixed(gain.shape)]
    in_specs += [pl.BlockSpec((1, width, out_width), lambda i, p: (layer, 0, 0))] * 3
    in_specs += [fixed(biases[0].shape)] * 3
    in_specs += [pl.BlockSpec((tile, HEAD_DIM), spot)] * 2
    args = [*pieces, gain, *weights, *biases, cos, sin]
    aliases = {}
    if prior is not None:
        aliases = {1 + len(args) + k: k for k in range(3)}
        in_specs += [pl.BlockSpec(memory_space=pl.ANY)] * 3
        args += list(prior)
    return pl.pallas_call(
        functools.partial(qkv_kernel, layer, norm, len(pieces)),
        out_shape=tuple(jax.ShapeDtypeStruct((block, out_width), jnp.bfloat16) for _ in range(3)),
        grid_spec=pltpu.PrefetchScalarGridSpec(
            num_scalar_prefetch=1, grid=(steps,), in_specs=in_specs,
            out_specs=tuple(pl.BlockSpec((tile, out_width), spot) for _ in range(3)),
            scratch_shapes=[pltpu.VMEM((tile, width), jnp.bfloat16)] if len(pieces) > 1 else []),
        input_output_aliases=aliases,
        compiler_params=pltpu.CompilerParams(dimension_semantics=("arbitrary",), vmem_limit_bytes=48 << 20),
        cost_estimate=pl.CostEstimate(flops=6 * steps * tile * width * out_width, bytes_accessed=6 * width * out_width, transcendentals=0),
    )(place, *args)


def put_kernel(n_pieces, place_ref, *refs):
    select_piece(pl.program_id(0), refs[:n_pieces], refs[-1])


def put_rows(place, pieces, block, prior=None):
    tile, width = pieces[0].shape
    steps = place.shape[0]
    args = [*pieces] + ([] if prior is None else [prior])
    return pl.pallas_call(
        functools.partial(put_kernel, len(pieces)),
        out_shape=jax.ShapeDtypeStruct((block, width), pieces[0].dtype),
        grid_spec=pltpu.PrefetchScalarGridSpec(
            num_scalar_prefetch=1, grid=(steps,),
            in_specs=piece_specs(pieces, tile) + ([] if prior is None else [pl.BlockSpec(memory_space=pl.ANY)]),
            out_specs=pl.BlockSpec((tile, width), lambda i, p: (p[i], 0))),
        input_output_aliases={} if prior is None else {1 + len(pieces): 0},
        compiler_params=pltpu.CompilerParams(dimension_semantics=("arbitrary",), vmem_limit_bytes=24 << 20),
        cost_estimate=pl.CostEstimate(flops=10 ** 9, bytes_accessed=4 * steps * tile * width, transcendentals=0),
    )(place, *args)


def normalize(hidden_f, gain):
    variance = jnp.mean(hidden_f * hidden_f, axis=-1, keepdims=True)
    return (hidden_f * lax.rsqrt(variance + 1e-6) * gain.astype(jnp.float32)).astype(jnp.bfloat16)


def rope_tables(positions):
    inv_freq = 1.0 / (1000000.0 ** (jnp.arange(0, HEAD_DIM, 2, dtype=jnp.float32) / HEAD_DIM))
    angles = positions.astype(jnp.float32)[:, None] * inv_freq[None, :]
    cos, sin = jnp.cos(angles), jnp.sin(angles)
    return jnp.concatenate([cos, cos], 1), jnp.concatenate([-sin, sin], 1)


def solution(mesh):
    tp_size = mesh.shape['tp']
    cp_size = mesh.shape['cp']
    swap_x = [(c, c ^ 2) for c in range(cp_size)]
    swap_core = [(c, c ^ 1) for c in range(cp_size)]
    to_later_chip = [(0, 2), (1, 3)]
    to_later_core = [(0, 1), (2, 3)]
    share_late_chip = [(2, 3), (3, 2)]

    def swap_tp(d):
        return [(t, t ^ d) for t in range(tp_size)]

    def local_step(x_in, positions, attn_gain, mlp_gain, w_query, b_query, w_key, b_key, w_value, b_value, w_out, w_gate, w_up, w_down):
        block, width = x_in.shape
        own = block // tp_size
        kv_width = w_key.shape[2]
        pair_width = kv_width // 2
        ffn_half = w_gate.shape[2] // 2
        col_half = width // 2
        t_idx = lax.axis_index('tp').astype(jnp.int32)
        c_idx = lax.axis_index('cp').astype(jnp.int32)
        x_idx = c_idx // 2
        core = c_idx % 2
        core_flag = core.reshape(1)

        def trade(w):
            return lax.ppermute(w, 'cp', swap_core)

        def after(value, *events):
            return lax.optimization_barrier((value,) + events)[0]

        def gather_out(part):
            return lax.all_gather(part, 'tp', axis=0, tiled=True)

        def out_part(layer):
            return lax.dynamic_slice(w_out, (layer, 0, core * col_half), (1, kv_width, col_half))[0]

        def down_part(layer):
            return lax.dynamic_slice(w_down, (layer, x_idx * ffn_half, core * col_half), (1, ffn_half, col_half))[0]

        def wide_part(layer, *events):
            w_gate_l, w_up_l = lax.optimization_barrier((w_gate, w_up) + events)[:2]
            cut = lambda w: lax.dynamic_slice(jnp.swapaxes(w, 1, 2), (layer, x_idx * ffn_half, 0), (1, ffn_half, width))[0]
            return jnp.where(core == 0, cut(w_gate_l), cut(w_up_l))

        def gather_stack(part):
            return lax.all_gather(part, 'tp', axis=0)

        def join_cols(mine, other):
            return jnp.where(core == 0, jnp.concatenate([mine, other], 1), jnp.concatenate([other, mine], 1))

        def places(k, chunks):
            return jnp.stack([(t_idx ^ d) * chunks + k for d in range(tp_size)])

        def spread_heads(attn):
            pieces = []
            for d in range(tp_size):
                piece = lax.dynamic_slice_in_dim(attn, (t_idx ^ d) * own, own, 0)
                pieces.append(lax.ppermute(piece, 'tp', swap_tp(d)) if d else piece)
            return pieces

        def collect_heads(groups):
            return jnp.concatenate([g[d] for d in range(tp_size) for g in groups], 1)

        def by_distance(gathered):
            return jnp.concatenate([lax.dynamic_slice_in_dim(gathered, (t_idx ^ d) * kv_width, kv_width, 0) for d in range(tp_size)], 0)

        def delta_of(distance):
            return (((c_idx ^ distance) - c_idx) * block).astype(jnp.int32)

        def attend(queries, packs, window, out_all, wide_all):
            near = jnp.stack([delta_of(0), delta_of(1)])
            far = jnp.stack([delta_of(2), delta_of(3)])
            nearby = [lax.ppermute(p, 'cp', to_later_core) for p in packs]
            remote = []
            for pack in packs:
                remote.append(lax.ppermute(pack, 'cp', to_later_chip))

            def local(g, first, count, held):
                return flash(held, (packs[g], nearby[g]), near, window, first, count, final=False, units=1.5)

            both = local(0, 0, 2, queries)
            held, both[1] = lax.optimization_barrier((queries, both[1]))
            third = local(1, 2, 1, held)
            held, third[1], far0 = lax.optimization_barrier((held, third[1], remote[0]))
            sources = (far0, lax.ppermute(far0, 'cp', share_late_chip))
            fourth = local(1, 3, 1, held)

            def finish(head, carry, start, held):
                return flash(held, sources if head < 2 else other, far, window, head, 1, carry=carry, start=start, units=2.0)

            held, fourth[1] = lax.optimization_barrier((held, fourth[1]))
            outs = [finish(0, both, 0, held)]
            far1, held, outs[0] = lax.optimization_barrier((remote[1], held, outs[0]))
            other = (far1, lax.ppermute(far1, 'cp', share_late_chip))
            sent = [spread_heads(outs[0])]
            outs.append(finish(1, both, 1, held))
            held, outs[1] = lax.optimization_barrier((held, outs[1]))
            sent.append(spread_heads(outs[1]))
            outs.append(finish(2, third, 0, held))
            held, outs[2], out_all, wide_all = lax.optimization_barrier((held, outs[2], out_all, wide_all))
            out_w = (out_all, trade(out_all))
            wide_w = (wide_all, trade(wide_all))
            sent.append(spread_heads(outs[2]))
            sent.append(spread_heads(finish(3, fourth, 0, held)))
            return collect_heads(sent), out_w, wide_w

        cos_tab, sin_tab = rope_tables(positions)
        residual = lax.dynamic_slice_in_dim(x_in, t_idx * own, own, 0).astype(jnp.float32)
        projections = ((w_query, w_key, w_value), (b_query, b_key, b_value))
        out_all = by_distance(gather_out(out_part(0)))
        chunks = 2
        piece = own // chunks
        fresh = qkv(0, True, jnp.arange(block // piece, dtype=jnp.int32), (x_in,), attn_gain, *projections, cos_tab, sin_tab, block, tile=piece)
        wide_all = gather_stack(wide_part(0, fresh[0]))
        down_all = gather_stack(after(down_part(0), fresh[0]))
        caches = []
        for layer in range(2):
            window = block * cp_size if layer == 0 else WINDOW
            queries, packs = fresh[0], fresh[1:]
            heads_all, out_w, wide_w = attend(queries, packs, window, out_all, wide_all)
            proj = join_cols(*(jnp.dot(heads_all, w, preferred_element_type=jnp.float32) for w in out_w))
            mid = (residual + proj).astype(jnp.bfloat16)
            h_mid = normalize(mid.astype(jnp.float32), mlp_gain[layer])
            guests = [lax.ppermute(h_mid[k * piece:(k + 1) * piece], 'cp', swap_x) for k in range(chunks)]
            h_mid, down_all = lax.optimization_barrier((h_mid, down_all))
            down_w = (down_all, trade(down_all))
            if layer == 0:
                out_all = by_distance(gather_out(after(out_part(1), h_mid)))
                down_all = gather_stack(after(down_part(1), h_mid))
            mine = mlp(core_flag, h_mid, *wide_w, *down_w, residual=mid)
            guests[0], mine = lax.optimization_barrier((guests[0], mine))
            guest_out = mlp(core_flag, guests[0], *wide_w, *down_w)
            back = [lax.ppermute(guest_out, 'cp', swap_x)]
            guests[1], guest_out = lax.optimization_barrier((guests[1], guest_out))
            guest_last = mlp(core_flag, guests[1], *wide_w, *down_w)
            back.append(lax.ppermute(guest_last, 'cp', swap_x))
            back[0], guest_last = lax.optimization_barrier((back[0], guest_last))
            heads = lambda at: jnp.concatenate([p[:, at:at + pair_width] for p in packs], 1).reshape(block, -1, HEAD_DIM)
            held = [heads(0), heads(pair_width)]
            rest, result, last = [], None, back[1]
            held[0], held[1], last = lax.optimization_barrier((held[0], held[1], last))
            caches += held
            if layer == 0:
                wide_next, last = lax.optimization_barrier((wide_part(1, guest_last), last))
            for k in range(chunks):
                from_guest = back[0] if k == 0 else last
                hidden = (mine[k * piece:(k + 1) * piece] + from_guest.astype(jnp.float32)).astype(jnp.bfloat16)
                rest.append(hidden.astype(jnp.float32))
                rows = normalize(rest[k], attn_gain[1]) if layer == 0 else hidden
                by_y = lax.ppermute(rows, 'tp', swap_tp(1))
                by_z = lax.ppermute(rows, 'tp', swap_tp(2))
                if k == 0:
                    by_y, by_z, last = lax.optimization_barrier((by_y, by_z, last))
                elif layer == 0:
                    by_y, by_z, result[0] = lax.optimization_barrier((by_y, by_z, result[0]))
                else:
                    by_y, by_z, result = lax.optimization_barrier((by_y, by_z, result))
                half = piece // 2
                pieces = (rows, by_y, by_z, lax.ppermute(by_y[:half], 'tp', swap_tp(2)), lax.ppermute(by_z[half:], 'tp', swap_tp(1)))
                if layer == 0:
                    result = list(qkv(1, False, places(k, chunks), pieces, attn_gain, *projections, cos_tab, sin_tab, block, prior=result, tile=piece))
                else:
                    result = put_rows(places(k, chunks), pieces, block, result)
            if layer == 0:
                fresh = result
                residual = jnp.concatenate(rest, 0)
                wide_all = gather_stack(after(wide_next, fresh[0], down_all))
        return result, caches[0], caches[1], caches[2], caches[3]

    weight_col = P(None, None, 'tp')
    bias_col = P(None, 'tp')
    weight_row = P(None, 'tp', None)
    replicated = P(None, None)
    cache_spec = P('cp', 'tp', None)
    in_specs = (P('cp', None), P('cp'), replicated, replicated, weight_col, bias_col, weight_col, bias_col, weight_col, bias_col, weight_row, weight_col, weight_col, weight_row)
    out_specs = (P('cp', None), cache_spec, cache_spec, cache_spec, cache_spec)
    return jax.shard_map(local_step, mesh=mesh, in_specs=in_specs, out_specs=out_specs, check_vma=False)
```
